256 devices in a mesh: depth: 32 (over x, y, core), rays: 8 (over z).
Axes of the slice: x: 4, y: 4, z: 8, core: 2. Of those that a mesh axis runs over, the one named last changes fastest.
Arguments:
- density: float32 [1024, 131072], P('depth', 'rays'), may hold values from 4.8828125e-05 to 0.80390625
- radiance: float32 [3, 1024, 131072], P(None, 'depth', 'rays'), may hold values from 0 to 1
- target: float32 [3, 131072], P(None, 'rays'), may hold values from 0 to 1
Outputs:
- grad_density: float32 [1024, 131072], P('depth', 'rays')
- loss_mean: float32 [], replicated
The draws below stay inside these ranges and needn't reach their ends.
All inputs are finite; a program needn't handle non-finite values.
Results may differ from the reference program's by a relative error of at most 0.0003.
Values sent between devices are 32-bit elements; how exact they have to be, the bound alone decides.
No kernel may reach another device: no remote copies, remote signals or barrier semaphores. Data moves between devices by JAX's collectives and lax.ppermute only.
A program may use at most 128 MiB of HBM per device.

```python
import math
import jax
import jax.numpy as jnp
from jax import lax

POINT_COUNT = 1024
RAYS = 131072


def draw_density(key, part):
    base_key = jax.random.fold_in(key, 7301)
    first_key, second_key, third_key, fourth_key = jax.random.split(base_key, 4)
    starting_shift_amount = jnp.exp(jax.random.uniform(first_key, (POINT_COUNT, RAYS), jnp.float32, math.log(0.1), math.log(2.0)))
    multiplier_coefficient = jnp.exp(jax.random.uniform(second_key, (1, RAYS), jnp.float32, math.log(0.5), math.log(2.0)))
    location_numbers = jax.random.randint(third_key, (2, RAYS), 0, POINT_COUNT)
    elevation_levels = jax.random.uniform(fourth_key, (2, RAYS), jnp.float32, 0.15, 0.4)
    vertical_element = jnp.arange(POINT_COUNT, dtype=jnp.int32)[:, None]
    packet_clusters = jnp.where(vertical_element == location_numbers[0:1], elevation_levels[0:1], 0.0) + jnp.where(vertical_element == location_numbers[1:2], elevation_levels[1:2], 0.0)
    return (starting_shift_amount * multiplier_coefficient / POINT_COUNT + packet_clusters).astype(jnp.float32)


def shard_levels(stream_key, dims, pieces, smallest, high):
    def one(dim, blocks):
        draws = jax.random.uniform(jax.random.fold_in(jax.random.fold_in(stream_key, 6), dim), (blocks,), jnp.float32, smallest / len(pieces), high / len(pieces))
        return jnp.repeat(jnp.exp(draws), dims[dim] // blocks).reshape((-1,) + (1,) * (len(dims) - dim - 1))

    gain = one(*pieces[0])
    for cut in pieces[1:]:
        gain = gain * one(*cut)
    return gain


def setup_inputs(seed: int = 0) -> dict:
    keys = jax.random.split(jax.random.key(seed), 4)
    density = draw_density(jax.random.fold_in(keys[3], 71), 0)
    radiance = jnp.clip(1.0 * jax.random.uniform(keys[1], (3, POINT_COUNT, RAYS), jnp.float32) ** shard_levels(keys[1], (3, POINT_COUNT, RAYS), ((1, 32), (2, 8)), -0.2, 0.2), 0.0, 1.0)
    target = jnp.clip(1.0 * jax.random.uniform(keys[2], (3, RAYS), jnp.float32) ** shard_levels(keys[2], (3, RAYS), ((1, 8),), -0.2, 0.2), 0.0, 1.0)
    return dict(density=density, radiance=radiance, target=target)


def render_block(density, radiance, target):
    width = density.shape[1]
    zero_row = jnp.zeros((1, width), jnp.float32)
    zero_plane = jnp.zeros((3, 1, width), jnp.float32)
    sample_density = 0.5 * (density + jnp.concatenate([density[1:], zero_row], axis=0))
    sample_color = 0.5 * (radiance + jnp.concatenate([radiance[:, 1:], zero_plane], axis=1))
    running = jnp.cumsum(sample_density, axis=0)
    optical = jnp.concatenate([zero_row, running[:-1]], axis=0)
    transmit = jnp.exp(-optical)
    weight = transmit * (-jnp.expm1(-sample_density))
    emitted = weight[None] * sample_color
    prefix = jnp.cumsum(emitted, axis=1)
    pixel_color = prefix[:, -1]
    remaining = pixel_color[:, None, :] - prefix
    residual_grad = 2.0 * (pixel_color - target)
    transmit_next = transmit * jnp.exp(-sample_density)
    bracket = transmit_next[None] * sample_color - remaining
    sample_grad = jnp.sum(residual_grad[:, None, :] * bracket, axis=0)
    shifted = jnp.concatenate([zero_row, sample_grad[:-1]], axis=0)
    grad_block = 0.5 * (sample_grad + shifted)
    error_term = pixel_color - target
    return grad_block, jnp.sum(error_term * error_term)


def reference(density, radiance, target):
    block_rays = math.gcd(RAYS, 4096)
    block_count = RAYS // block_rays

    def render_one(block_index):
        start = (block_index * block_rays).astype(jnp.int32)
        part_density = lax.dynamic_slice_in_dim(density, start, block_rays, 1)
        part_radiance = lax.dynamic_slice_in_dim(radiance, start, block_rays, 2)
        part_target = lax.dynamic_slice_in_dim(target, start, block_rays, 1)
        return render_block(part_density, part_radiance, part_target)

    block_grads, losses = lax.map(render_one, jnp.arange(block_count, dtype=jnp.int32))
    grad_density = jnp.moveaxis(block_grads, 0, 1).reshape(POINT_COUNT, RAYS)
    loss_mean = jnp.sum(losses) / (3.0 * RAYS)
    return grad_density, loss_mean
```

```python
import jax
import jax.numpy as jnp
from jax import lax
from jax.experimental import pallas as pl
from jax.experimental.pallas import tpu as pltpu
from jax.sharding import PartitionSpec as P

SLABS = 32
SAMPLES = 32
EIGHTS = SAMPLES // 8
TILES = 128
LANES = 128
OWNED = TILES // SLABS
GROUP = 8
SENT = 12
LOSS = 6 * OWNED
ANSWER = 8 * OWNED
F32 = jnp.float32
MIB = 1 << 20
LARGE = 59
WHOLE = pl.BlockSpec(memory_space=pltpu.VMEM)
FAR = pl.BlockSpec(memory_space=pltpu.HBM)


def call(kernel, name, in_specs, out_specs, out_shape, scratch, mib, flops=0):
    return pl.pallas_call(
        kernel,
        in_specs=in_specs,
        out_specs=out_specs,
        out_shape=out_shape,
        scratch_shapes=scratch,
        compiler_params=pltpu.CompilerParams(vmem_limit_bytes=mib * MIB),
        cost_estimate=pl.CostEstimate(flops=flops, bytes_accessed=8 * MIB, transcendentals=0),
        name=name,
    )


def tiled_view(block):
    lead = block.shape[:-2]
    cut = block.reshape(*lead, EIGHTS, 8, TILES, LANES)
    return jnp.swapaxes(cut, -3, -2).reshape(-1, TILES * 8, LANES)


def untiled_view(block):
    cut = block.reshape(EIGHTS, TILES, 8, LANES)
    return jnp.swapaxes(cut, 1, 2).reshape(SAMPLES, TILES * LANES)


def sample_place(sample, base):
    return pl.ds(pl.multiple_of(base * 8, 64) + sample % 8, GROUP, stride=8)


def sample_row(ref, channel, sample, base):
    return ref[channel * EIGHTS + sample // 8, sample_place(sample, base), :]


def fetches(pairs, sems):
    chunks = sems.shape[0]
    size = TILES * 8 // chunks
    return [
        [
            pltpu.make_async_copy(a.at[:, pl.ds(k * size, size)], b.at[:, pl.ds(k * size, size)], sems.at[k, n])
            for n, (a, b) in enumerate(pairs)
        ]
        for k in range(chunks)
    ]


def start_all(copies):
    for some in copies:
        for copy in some:
            copy.start()


def wait_all(copies):
    for some in copies:
        for copy in some:
            copy.wait()


def in_chunks(arrivals, departures, count, one):
    start_all(arrivals)
    each = count // len(arrivals)
    for k, some in enumerate(arrivals):
        wait_all([some])
        lax.fori_loop(k * each, (k + 1) * each, one, 0)
        start_all([departures[k]])
    wait_all(departures)


def inner_kernel(density_in, radiance_in, out, density, radiance, sent, sems, out_sems):
    chunks = sems.shape[0]
    owners = SLABS // chunks

    def one_group(group, carry):
        base = pl.multiple_of(group * GROUP, GROUP)
        first = here = sample_row(density, 0, 0, base)
        color = [sample_row(radiance, c, 0, base) for c in range(3)]
        before = first_color = color
        doubled = jnp.zeros((GROUP, LANES), F32)
        total = None
        half = None
        for i in range(SAMPLES - 1):
            nxt = sample_row(density, 0, i + 1, base)
            after = [sample_row(radiance, c, i + 1, base) for c in range(3)]
            if i == 0:
                total = [0.5 * (color[c] + after[c]) for c in range(3)]
            else:
                total = [total[c] + half * (after[c] - before[c]) for c in range(3)]
            doubled = doubled + (here + nxt)
            half = 0.5 * jnp.exp(-0.5 * doubled)
            before, color, here = color, after, nxt
        known = [total[c] - half * before[c] for c in range(3)]
        parts = [doubled, here, first] + known + color + first_color
        for q in range(SENT):
            for k in range(GROUP // OWNED):
                owner = group * (GROUP // OWNED) + k
                sent[owner, q * OWNED : (q + 1) * OWNED, :] = parts[q][k * OWNED : (k + 1) * OWNED, :]
        return carry

    arrivals = fetches([(density_in, density), (radiance_in, radiance)], sems)
    departures = [
        [
            pltpu.make_async_copy(
                sent.at[pl.ds(k * owners, owners)], out.at[pl.ds(k * owners, owners)], out_sems.at[k]
            )
        ]
        for k in range(chunks)
    ]
    in_chunks(arrivals, departures, TILES // GROUP, one_group)


def inner(density, radiance, chunks=8):
    shape = (SLABS, SENT * OWNED, LANES)
    return call(
        inner_kernel,
        "slab_inner",
        [FAR, FAR],
        FAR,
        jax.ShapeDtypeStruct(shape, F32),
        [
            pltpu.VMEM((EIGHTS, TILES * 8, LANES), F32),
            pltpu.VMEM((3 * EIGHTS, TILES * 8, LANES), F32),
            pltpu.VMEM(shape, F32),
            pltpu.SemaphoreType.DMA((chunks, 2)),
            pltpu.SemaphoreType.DMA((chunks,)),
        ],
        LARGE,
    )(density, radiance)


def scan_kernel(owner, slabs, target, out):
    def value(s, q):
        return slabs[s, q * OWNED : (q + 1) * OWNED, :]

    zero = jnp.zeros((OWNED, LANES), F32)
    start = zero
    pixel = [zero] * 3
    offsets, befores, ends = [], [], []
    for s in range(SLABS):
        more = s < SLABS - 1
        doubled = value(s, 0)
        depth = 0.5 * (doubled + value(s, 1) + (value(s + 1, 2) if more else zero))
        half = 0.5 * jnp.exp(-0.5 * doubled)
        behind = 0.5 * jnp.exp(-depth)
        offset = jnp.exp(-start)
        end = []
        befores.append(pixel)
        following = []
        for c in range(3):
            after = value(s + 1, 9 + c) if more else zero
            last = value(s, 3 + c) + half * after
            end.append(offset * last)
            following.append(pixel[c] + offset * (last - behind * (value(s, 6 + c) + after)))
        pixel = following
        offsets.append(offset)
        ends.append(end)
        start = start + depth
    first = owner[0] * (OWNED * LANES)
    error = []
    for c in range(3):
        rows = [
            target[c : c + 1, pl.ds(pl.multiple_of(first + k * LANES, LANES), LANES)]
            for k in range(OWNED)
        ]
        error.append(pixel[c] - jnp.concatenate(rows, axis=0))
    residual = [2.0 * e for e in error]
    loss = error[0] * error[0] + error[1] * error[1] + error[2] * error[2]
    previous = zero
    for s in range(SLABS):
        left = [residual[c] * (pixel[c] - befores[s][c]) for c in range(3)]
        left = left[0] + left[1] + left[2]
        last = [residual[c] * ends[s][c] for c in range(3)]
        last = last[0] + last[1] + last[2] - left
        answer = [offsets[s] * residual[c] for c in range(3)]
        answer += [left, 0.5 * (left - previous), 0.5 * (left - last), loss, zero]
        for q, part in enumerate(answer):
            out[s, q * OWNED : (q + 1) * OWNED, :] = part
        previous = last


def scan_slabs(owner, slabs, target):
    return call(
        scan_kernel,
        "scan_slabs",
        [pl.BlockSpec(memory_space=pltpu.SMEM), WHOLE, WHOLE],
        WHOLE,
        jax.ShapeDtypeStruct((SLABS, ANSWER, LANES), F32),
        [],
        6,
    )(owner, slabs, target)


def halves_kernel(density_in, radiance_in, out, density, radiance, halves, sems, out_sems):
    def one_group(group, carry):
        base = pl.multiple_of(group * GROUP, GROUP)
        here = sample_row(density, 0, 0, base)
        color = [sample_row(radiance, c, 0, base) for c in range(3)]
        before = color
        doubled = jnp.zeros((GROUP, LANES), F32)
        half = None
        for i in range(SAMPLES):
            store = half
            if i < SAMPLES - 1:
                after = [sample_row(radiance, c, i + 1, base) for c in range(3)]
                if i == 0:
                    half = [0.25 * (color[c] + after[c]) for c in range(3)]
                    store = half
                else:
                    transmit = 0.25 * jnp.exp(-0.5 * doubled)
                    new = [half[c] + transmit * (after[c] - before[c]) for c in range(3)]
                    store = [half[c] + new[c] for c in range(3)]
                    half = new
                nxt = sample_row(density, 0, i + 1, base)
                doubled = doubled + (here + nxt)
                here, before, color = nxt, color, after
            for c in range(3):
                halves[c * EIGHTS + i // 8, sample_place(i, base), :] = store[c]
        return carry

    arrivals = fetches([(density_in, density), (radiance_in, radiance)], sems)
    in_chunks(arrivals, fetches([(halves, out)], out_sems), TILES // GROUP, one_group)


def halves_of(density, radiance, chunks=8):
    shape = (3 * EIGHTS, TILES * 8, LANES)
    return call(
        halves_kernel,
        "slab_halves",
        [FAR, FAR],
        FAR,
        jax.ShapeDtypeStruct(shape, F32),
        [
            pltpu.VMEM((EIGHTS, TILES * 8, LANES), F32),
            pltpu.VMEM(shape, F32),
            pltpu.VMEM(shape, F32),
            pltpu.SemaphoreType.DMA((chunks, 2)),
            pltpu.SemaphoreType.DMA((chunks, 1)),
        ],
        LARGE,
        1_000_000_000,
    )(density, radiance)


def loss_kernel(back, out):
    total = back[0, LOSS : LOSS + OWNED, :]
    for s in range(1, SLABS):
        total = total + back[s, LOSS : LOSS + OWNED, :]
    total = jnp.sum(total, axis=0, keepdims=True)
    for z in range(out.shape[0]):
        out[z] = total


def tile_loss(back, count):
    return call(
        loss_kernel,
        "tile_loss",
        [WHOLE],
        WHOLE,
        jax.ShapeDtypeStruct((count, 1, LANES), F32),
        [],
        4,
    )(back)


def gradient_kernel(halves_in, back, out, halves, held, sems, out_sems):
    sample = lax.broadcasted_iota(jnp.int32, (8, LANES), 0)

    def one_owner(owner, carry):
        for k in range(OWNED):
            rows = pl.ds(pl.multiple_of(owner * (OWNED * 8), OWNED * 8) + k * 8, 8)
            known = [
                jnp.broadcast_to(back[owner, q * OWNED + k : q * OWNED + k + 1, :], (8, LANES))
                for q in range(6)
            ]
            for a in range(EIGHTS):
                value = known[0] * halves[a, rows, :]
                value += known[1] * halves[EIGHTS + a, rows, :]
                value += known[2] * halves[2 * EIGHTS + a, rows, :]
                left = known[3]
                if a == 0:
                    left = jnp.where(sample == 0, known[4], left)
                if a == EIGHTS - 1:
                    left = jnp.where(sample == 7, known[5], left)
                held[a, rows, :] = value - left
        return carry

    arrivals = fetches([(halves_in, halves)], sems)
    in_chunks(arrivals, fetches([(held, out)], out_sems), SLABS, one_owner)


def gradient(halves, back, chunks=8):
    shape = (EIGHTS, TILES * 8, LANES)
    return call(
        gradient_kernel,
        "slab_gradient",
        [FAR, WHOLE],
        FAR,
        jax.ShapeDtypeStruct(shape, F32),
        [
            pltpu.VMEM((3 * EIGHTS, TILES * 8, LANES), F32),
            pltpu.VMEM(shape, F32),
            pltpu.SemaphoreType.DMA((chunks, 1)),
            pltpu.SemaphoreType.DMA((chunks, 1)),
        ],
        LARGE,
        1_000_000_000,
    )(halves, back)


def on_device(density, radiance, target):
    density, radiance = tiled_view(density), tiled_view(radiance)
    owner = lax.axis_index("depth").astype(jnp.int32)[None]
    slabs = lax.all_to_all(inner(density, radiance), "depth", 0, 0, tiled=True)
    answers = scan_slabs(owner, slabs, target)
    back = lax.all_to_all(answers, "depth", 0, 0, tiled=True)
    halves = halves_of(density, radiance)
    zs = lax.axis_size("rays")
    losses = lax.all_to_all(tile_loss(back, zs), "rays", 0, 0, tiled=True)
    grad = gradient(halves, back)
    loss_mean = jnp.sum(losses) / (3.0 * zs * TILES * LANES)
    return untiled_view(grad), loss_mean


def solution(mesh):
    in_specs = (P("depth", "rays"), P(None, "depth", "rays"), P(None, "rays"))
    out_specs = (P("depth", "rays"), P())
    return jax.shard_map(
        on_device, mesh=mesh, in_specs=in_specs, out_specs=out_specs, check_vma=False
    )
```

```python
import functools

import jax
import jax.numpy as jnp
from jax import lax
from jax.experimental import pallas as pl
from jax.experimental.pallas import tpu as pltpu
from jax.sharding import PartitionSpec as P

SLABS = 32
SAMPLES = 32
EIGHTS = SAMPLES // 8
TILES = 128
LANES = 128
OWNED = TILES // SLABS
GROUP = 8
SENT = 12
LOSS = 6 * OWNED
ANSWER = LOSS + 1
F32 = jnp.float32
MIB = 1 << 20
INNER_MIB, HALVES_MIB, GRADIENT_MIB = 52, 49.5, 50
NEAR = 48
WHOLE = pl.BlockSpec(memory_space=pltpu.VMEM)
FAR = pl.BlockSpec(memory_space=pltpu.HBM)


def call(kernel, name, in_specs, out_specs, out_shape, scratch, mib, flops=0):
    return pl.pallas_call(
        kernel,
        in_specs=in_specs,
        out_specs=out_specs,
        out_shape=out_shape,
        scratch_shapes=scratch,
        compiler_params=pltpu.CompilerParams(vmem_limit_bytes=int(mib * MIB)),
        cost_estimate=pl.CostEstimate(flops=flops, bytes_accessed=1024, transcendentals=0),
        name=name,
    )


def tiled_view(block):
    lead = block.shape[:-2]
    cut = block.reshape(*lead, EIGHTS, 8, TILES, LANES)
    return jnp.swapaxes(cut, -3, -2).reshape(-1, TILES * 8, LANES)


def untiled_view(block):
    cut = block.reshape(EIGHTS, TILES, 8, LANES)
    return jnp.swapaxes(cut, 1, 2).reshape(SAMPLES, TILES * LANES)


def sample_place(sample, base):
    return pl.ds(pl.multiple_of(base * 8, 64) + sample % 8, GROUP, stride=8)


def sample_row(ref, channel, sample, base):
    return ref[channel * EIGHTS + sample // 8, sample_place(sample, base), :]


def fetches(pairs, sems):
    chunks = sems.shape[0]
    size = pairs[0][0].shape[1] // chunks
    return [
        [
            pltpu.make_async_copy(a.at[:, pl.ds(k * size, size)], b.at[:, pl.ds(k * size, size)], sems.at[k, n])
            for n, (a, b) in enumerate(pairs)
        ]
        for k in range(chunks)
    ]


def start_all(copies):
    for some in copies:
        for copy in some:
            copy.start()


def wait_all(copies):
    for some in copies:
        for copy in some:
            copy.wait()


def in_chunks(arrivals, departures, count, one):
    start_all(arrivals)
    each = count // len(arrivals)
    for k, some in enumerate(arrivals):
        wait_all([some])
        lax.fori_loop(k * each, (k + 1) * each, one, 0)
        if departures:
            start_all([departures[k]])
    if departures:
        wait_all(departures)


def inner_kernel(owner, density_in, radiance_in, sent, density, radiance, sems):
    def one_group(group, carry):
        base = pl.multiple_of(group * GROUP, GROUP)
        first = here = sample_row(density, 0, 0, base)
        color = [sample_row(radiance, c, 0, base) for c in range(3)]
        before = first_color = color
        doubled = jnp.zeros((GROUP, LANES), F32)
        total = None
        half = None
        for i in range(SAMPLES - 1):
            nxt = sample_row(density, 0, i + 1, base)
            after = [sample_row(radiance, c, i + 1, base) for c in range(3)]
            if i == 0:
                total = [0.5 * (color[c] + after[c]) for c in range(3)]
            else:
                total = [total[c] + half * (after[c] - before[c]) for c in range(3)]
            doubled = doubled + (here + nxt)
            half = 0.5 * jnp.exp(-0.5 * doubled)
            before, color, here = color, after, nxt
        known = [total[c] - half * before[c] for c in range(3)]
        parts = [doubled, here, first] + known + color + first_color
        for q in range(SENT):
            for k in range(GROUP // OWNED):
                owner = group * (GROUP // OWNED) + k
                sent[owner, q * OWNED : (q + 1) * OWNED, :] = parts[q][k * OWNED : (k + 1) * OWNED, :]
        return carry

    arrivals = fetches([(density_in, density), (radiance_in, radiance)], sems)
    in_chunks(arrivals, None, TILES // GROUP, one_group)


def inner(owner, density, radiance, chunks=8):
    shape = (SLABS, SENT * OWNED, LANES)
    return call(
        inner_kernel,
        "slab_inner",
        [pl.BlockSpec(memory_space=pltpu.SMEM), FAR, FAR],
        WHOLE,
        jax.ShapeDtypeStruct(shape, F32),
        [
            pltpu.VMEM((EIGHTS, TILES * 8, LANES), F32),
            pltpu.VMEM((3 * EIGHTS, TILES * 8, LANES), F32),
            pltpu.SemaphoreType.DMA((chunks, 2)),
        ],
        INNER_MIB,
    )(owner, density, radiance)


def scan_kernel(owner, slabs, target, out):
    def value(s, q):
        return slabs[s, q * OWNED : (q + 1) * OWNED, :]

    zero = jnp.zeros((OWNED, LANES), F32)
    start = zero
    pixel = [zero] * 3
    offsets, befores, ends = [], [], []
    for s in range(SLABS):
        more = s < SLABS - 1
        doubled = value(s, 0)
        depth = 0.5 * (doubled + value(s, 1) + (value(s + 1, 2) if more else zero))
        half = 0.5 * jnp.exp(-0.5 * doubled)
        behind = 0.5 * jnp.exp(-depth)
        offset = jnp.exp(-start)
        end = []
        befores.append(pixel)
        following = []
        for c in range(3):
            after = value(s + 1, 9 + c) if more else zero
            last = value(s, 3 + c) + half * after
            end.append(offset * last)
            following.append(pixel[c] + offset * (last - behind * (value(s, 6 + c) + after)))
        pixel = following
        offsets.append(offset)
        ends.append(end)
        start = start + depth
    first = owner[0] * (OWNED * LANES)
    error = []
    for c in range(3):
        rows = [
            target[c : c + 1, pl.ds(pl.multiple_of(first + k * LANES, LANES), LANES)]
            for k in range(OWNED)
        ]
        error.append(pixel[c] - jnp.concatenate(rows, axis=0))
    residual = [2.0 * e for e in error]
    loss = error[0] * error[0] + error[1] * error[1] + error[2] * error[2]
    loss = jnp.sum(loss, axis=0, keepdims=True)
    previous = zero
    for s in range(SLABS):
        left = [residual[c] * (pixel[c] - befores[s][c]) for c in range(3)]
        left = left[0] + left[1] + left[2]
        last = [residual[c] * ends[s][c] for c in range(3)]
        last = last[0] + last[1] + last[2] - left
        answer = [offsets[s] * residual[c] for c in range(3)]
        answer += [left, 0.5 * (left - previous), 0.5 * (left - last)]
        top = s * ANSWER
        for q, part in enumerate(answer):
            out[top + q * OWNED : top + (q + 1) * OWNED, :] = part
        out[top + LOSS : top + ANSWER, :] = loss
        previous = last


def scan_slabs(owner, slabs, target):
    return call(
        scan_kernel,
        "scan_slabs",
        [pl.BlockSpec(memory_space=pltpu.SMEM), WHOLE, WHOLE],
        WHOLE,
        jax.ShapeDtypeStruct((SLABS * ANSWER, LANES), F32),
        [],
        6,
    )(owner, slabs, target)


def halves_kernel(density_in, radiance_in, near, far, density, radiance, held, sems, out_sems):
    def one_group(out, first, group, carry):
        base = pl.multiple_of(group * GROUP, GROUP)
        here = sample_row(density, 0, 0, base)
        color = [sample_row(radiance, c, 0, base) for c in range(3)]
        before = color
        doubled = jnp.zeros((GROUP, LANES), F32)
        half = None
        for i in range(SAMPLES):
            store = half
            if i < SAMPLES - 1:
                after = [sample_row(radiance, c, i + 1, base) for c in range(3)]
                if i == 0:
                    half = [0.25 * (color[c] + after[c]) for c in range(3)]
                    store = half
                else:
                    transmit = 0.25 * jnp.exp(-0.5 * doubled)
                    new = [half[c] + transmit * (after[c] - before[c]) for c in range(3)]
                    store = [half[c] + new[c] for c in range(3)]
                    half = new
                nxt = sample_row(density, 0, i + 1, base)
                doubled = doubled + (here + nxt)
                here, before, color = nxt, color, after
            for c in range(3):
                out[c * EIGHTS + i // 8, sample_place(i, base - first), :] = store[c]
        return carry

    arrivals = fetches([(density_in, density), (radiance_in, radiance)], sems)
    departures = fetches([(held, far)], out_sems)
    start_all(arrivals)
    each = TILES // GROUP // len(arrivals)
    kept = NEAR // GROUP // each
    for k, some in enumerate(arrivals):
        wait_all([some])
        out, first = (near, 0) if k < kept else (held, NEAR)
        lax.fori_loop(k * each, (k + 1) * each, functools.partial(one_group, out, first), 0)
        if k >= kept:
            start_all([departures[k - kept]])
    wait_all(departures)


def halves_of(density, radiance, chunks=8):
    far = (3 * EIGHTS, (TILES - NEAR) * 8, LANES)
    return call(
        halves_kernel,
        "slab_halves",
        [FAR, FAR],
        [WHOLE, FAR],
        [
            jax.ShapeDtypeStruct((3 * EIGHTS, NEAR * 8, LANES), F32),
            jax.ShapeDtypeStruct(far, F32),
        ],
        [
            pltpu.VMEM((EIGHTS, TILES * 8, LANES), F32),
            pltpu.VMEM((3 * EIGHTS, TILES * 8, LANES), F32),
            pltpu.VMEM(far, F32),
            pltpu.SemaphoreType.DMA((chunks, 2)),
            pltpu.SemaphoreType.DMA((chunks * (TILES - NEAR) // TILES, 1)),
        ],
        HALVES_MIB,
        1_000_000_000,
    )(density, radiance)


def loss_kernel(back, near, out, near_out):
    total = jnp.sum(back[pl.ds(LOSS, SLABS, stride=ANSWER), :], axis=0, keepdims=True)
    for z in range(out.shape[0]):
        out[z] = total


def tile_loss(back, near, count):
    return pl.pallas_call(
        loss_kernel,
        in_specs=[WHOLE, WHOLE],
        out_specs=[WHOLE, WHOLE],
        out_shape=[
            jax.ShapeDtypeStruct((count, 1, LANES), F32),
            jax.ShapeDtypeStruct(near.shape, F32),
        ],
        input_output_aliases={1: 1},
        compiler_params=pltpu.CompilerParams(vmem_limit_bytes=8 * MIB),
        cost_estimate=pl.CostEstimate(flops=0, bytes_accessed=1024, transcendentals=0),
        name="tile_loss",
    )(back, near)


def gradient_kernel(near, far_in, back, out, far, held, sems, out_sems):
    sample = lax.broadcasted_iota(jnp.int32, (8, LANES), 0)

    def one_owner(halves, first, owner, carry):
        for k in range(OWNED):
            tile = owner * OWNED + k
            rows = pl.ds(pl.multiple_of(tile * 8, 8), 8)
            from_rows = pl.ds(pl.multiple_of((tile - first) * 8, 8), 8)
            known = [
                jnp.broadcast_to(back[pl.ds(owner * ANSWER + q * OWNED + k, 1), :], (8, LANES))
                for q in range(6)
            ]
            for a in range(EIGHTS):
                value = known[0] * halves[a, from_rows, :]
                value += known[1] * halves[EIGHTS + a, from_rows, :]
                value += known[2] * halves[2 * EIGHTS + a, from_rows, :]
                left = known[3]
                if a == 0:
                    left = jnp.where(sample == 0, known[4], left)
                if a == EIGHTS - 1:
                    left = jnp.where(sample == 7, known[5], left)
                held[a, rows, :] = value - left
        return carry

    arrivals = fetches([(far_in, far)], sems)
    departures = fetches([(held, out)], out_sems)
    start_all(arrivals)
    each = SLABS // len(departures)
    kept = len(departures) - len(arrivals)
    for k, some in enumerate(departures):
        if k >= kept:
            wait_all([arrivals[k - kept]])
        halves, first = (near, 0) if k < kept else (far, NEAR)
        lax.fori_loop(k * each, (k + 1) * each, functools.partial(one_owner, halves, first), 0)
        start_all([some])
    wait_all(departures)


def gradient(near, far, back, chunks=8):
    shape = (EIGHTS, TILES * 8, LANES)
    return call(
        gradient_kernel,
        "slab_gradient",
        [WHOLE, FAR, WHOLE],
        FAR,
        jax.ShapeDtypeStruct(shape, F32),
        [
            pltpu.VMEM((3 * EIGHTS, (TILES - NEAR) * 8, LANES), F32),
            pltpu.VMEM(shape, F32),
            pltpu.SemaphoreType.DMA((chunks * (TILES - NEAR) // TILES, 1)),
            pltpu.SemaphoreType.DMA((chunks, 1)),
        ],
        GRADIENT_MIB,
        1_000_000_000,
    )(near, far, back)


def on_device(density, radiance, target):
    density, radiance = tiled_view(density), tiled_view(radiance)
    owner = lax.axis_index("depth").astype(jnp.int32)[None]
    slabs = lax.all_to_all(inner(owner, density, radiance), "depth", 0, 0, tiled=True)
    answers = scan_slabs(owner, slabs, target)
    answers = answers.reshape(SLABS, ANSWER, 1, LANES)
    back = lax.all_to_all(answers, "depth", 0, 0, tiled=True).reshape(SLABS * ANSWER, LANES)
    near, far = halves_of(density, radiance)
    zs = lax.axis_size("rays")
    tile, near = tile_loss(back, near, zs)
    losses = lax.all_to_all(tile, "rays", 0, 0, tiled=True)
    grad = gradient(near, far, back)
    loss_mean = jnp.sum(losses) / (3.0 * zs * TILES * LANES)
    return untiled_view(grad), loss_mean


def solution(mesh):
    in_specs = (P("depth", "rays"), P(None, "depth", "rays"), P(None, "rays"))
    out_specs = (P("depth", "rays"), P())
    return jax.shard_map(
        on_device, mesh=mesh, in_specs=in_specs, out_specs=out_specs, check_vma=False
    )
```

```python
import functools

import jax
import jax.numpy as jnp
from jax import lax
from jax.experimental import pallas as pl
from jax.experimental.pallas import tpu as pltpu
from jax.sharding import PartitionSpec as P

SLABS = 32
SAMPLES = 32
EIGHTS = SAMPLES // 8
TILES = 128
LANES = 128
OWNED = TILES // SLABS
GROUP = 8
KNOWN = 12
SENT = 8
LOSS = 5 * OWNED
ANSWER = LOSS + 1
F32 = jnp.float32
MIB = 1 << 20
INNER_MIB, HALVES_MIB, GRADIENT_MIB = 52, 48, 50
NEAR = 48
WHOLE = pl.BlockSpec(memory_space=pltpu.VMEM)
FAR = pl.BlockSpec(memory_space=pltpu.HBM)


def call(kernel, name, in_specs, out_specs, out_shape, scratch, mib, flops=0):
    return pl.pallas_call(
        kernel,
        in_specs=in_specs,
        out_specs=out_specs,
        out_shape=out_shape,
        scratch_shapes=scratch,
        compiler_params=pltpu.CompilerParams(vmem_limit_bytes=int(mib * MIB)),
        cost_estimate=pl.CostEstimate(flops=flops, bytes_accessed=1024, transcendentals=0),
        name=name,
    )


def tiled_view(block):
    lead = block.shape[:-2]
    cut = block.reshape(*lead, EIGHTS, 8, TILES, LANES)
    return jnp.swapaxes(cut, -3, -2).reshape(-1, TILES * 8, LANES)


def untiled_view(block):
    cut = block.reshape(EIGHTS, TILES, 8, LANES)
    return jnp.swapaxes(cut, 1, 2).reshape(SAMPLES, TILES * LANES)


def sample_place(sample, base):
    return pl.ds(pl.multiple_of(base * 8, 64) + sample % 8, GROUP, stride=8)


def sample_row(ref, channel, sample, base):
    return ref[channel * EIGHTS + sample // 8, sample_place(sample, base), :]


def fetches(pairs, sems):
    chunks = sems.shape[0]
    size = pairs[0][0].shape[1] // chunks
    return [
        [
            pltpu.make_async_copy(a.at[:, pl.ds(k * size, size)], b.at[:, pl.ds(k * size, size)], sems.at[k, n])
            for n, (a, b) in enumerate(pairs)
        ]
        for k in range(chunks)
    ]


def start_all(copies):
    for some in copies:
        for copy in some:
            copy.start()


def wait_all(copies):
    for some in copies:
        for copy in some:
            copy.wait()


def in_chunks(arrivals, departures, count, one):
    start_all(arrivals)
    each = count // len(arrivals)
    for k, some in enumerate(arrivals):
        wait_all([some])
        lax.fori_loop(k * each, (k + 1) * each, one, 0)
        if departures:
            start_all([departures[k]])
    if departures:
        wait_all(departures)


def inner_kernel(slab, density_in, radiance_in, out, edge, density, radiance, sems):
    odd = slab[0] % 2 == 1
    def one_group(group, carry):
        base = pl.multiple_of(group * GROUP, GROUP)
        first = here = sample_row(density, 0, 0, base)
        color = [sample_row(radiance, c, 0, base) for c in range(3)]
        before = first_color = color
        doubled = jnp.zeros((GROUP, LANES), F32)
        total = None
        half = None
        for i in range(SAMPLES - 1):
            nxt = sample_row(density, 0, i + 1, base)
            after = [sample_row(radiance, c, i + 1, base) for c in range(3)]
            if i == 0:
                total = [0.5 * (color[c] + after[c]) for c in range(3)]
            else:
                total = [total[c] + half * (after[c] - before[c]) for c in range(3)]
            doubled = doubled + (here + nxt)
            half = 0.5 * jnp.exp(-0.5 * doubled)
            before, color, here = color, after, nxt
        known = [total[c] - half * before[c] for c in range(3)]
        rows = pl.ds(base, GROUP)
        for q, part in enumerate([doubled, here, first] + known + color + first_color):
            out[q, rows, :] = part
        edge[0, rows, :] = first
        for c in range(3):
            edge[1 + c, rows, :] = jnp.where(odd, first_color[c], color[c])
        return carry

    arrivals = fetches([(density_in, density), (radiance_in, radiance)], sems)
    in_chunks(arrivals, None, TILES // GROUP, one_group)


def inner(slab, density, radiance, chunks=8):
    return call(
        inner_kernel,
        "slab_inner",
        [pl.BlockSpec(memory_space=pltpu.SMEM), FAR, FAR],
        [WHOLE, WHOLE],
        [
            jax.ShapeDtypeStruct((KNOWN, TILES, LANES), F32),
            jax.ShapeDtypeStruct((4, TILES, LANES), F32),
        ],
        [
            pltpu.VMEM((EIGHTS, TILES * 8, LANES), F32),
            pltpu.VMEM((3 * EIGHTS, TILES * 8, LANES), F32),
            pltpu.SemaphoreType.DMA((chunks, 2)),
        ],
        INNER_MIB,
    )(slab, density, radiance)


def closing_kernel(slab, known, rim, out):
    def send(parity, parts_of):
        @pl.when(slab[0] % 2 == parity)
        def _():
            for group in range(TILES // GROUP):
                rows = pl.ds(group * GROUP, GROUP)
                for q, part in enumerate(parts_of(rows)):
                    for k in range(GROUP // OWNED):
                        owner = group * (GROUP // OWNED) + k
                        out[owner, q * OWNED : (q + 1) * OWNED, :] = part[k * OWNED : (k + 1) * OWNED, :]

    def even(rows):
        part = [known[q, rows, :] for q in range(KNOWN)]
        after = [rim[1 + c, rows, :] for c in range(3)]
        depth = 0.5 * (part[0] + part[1] + rim[0, rows, :])
        half = 0.5 * jnp.exp(-0.5 * part[0])
        behind = 0.5 * jnp.exp(-depth)
        color = [part[3 + c] + half * after[c] - behind * (part[6 + c] + after[c]) for c in range(3)]
        return [depth] + color + [part[2]] + part[9:]

    def odd(rows):
        return [known[q, rows, :] for q in (0, 3, 4, 5, 1, 6, 7, 8)]

    send(0, even)
    send(1, odd)


def closing(slab, known, rim):
    return call(
        closing_kernel,
        "slab_closing",
        [pl.BlockSpec(memory_space=pltpu.SMEM), WHOLE, WHOLE],
        WHOLE,
        jax.ShapeDtypeStruct((SLABS, SENT * OWNED, LANES), F32),
        [],
        6,
    )(slab, known, rim)


def scan_kernel(owner, slabs, target, out):
    def value(s, q):
        return slabs[s, q * OWNED : (q + 1) * OWNED, :]

    zero = jnp.zeros((OWNED, LANES), F32)
    start = zero
    pixel = [zero] * 3
    offsets, befores, ends = [], [], []
    for s in range(SLABS):
        offset = jnp.exp(-start)
        offsets.append(offset)
        befores.append(pixel)
        color = [value(s, 1 + c) for c in range(3)]
        if s % 2 == 0:
            depth = value(s, 0)
            ends.append(None)
        else:
            more = s < SLABS - 1
            depth = 0.5 * (value(s, 0) + value(s, 4) + (value(s + 1, 4) if more else zero))
            half = 0.5 * jnp.exp(-0.5 * value(s, 0))
            behind = 0.5 * jnp.exp(-depth)
            after = [value(s + 1, 5 + c) if more else zero for c in range(3)]
            color = [color[c] + half * after[c] for c in range(3)]
            ends.append([offset * color[c] for c in range(3)])
            color = [color[c] - behind * (value(s, 5 + c) + after[c]) for c in range(3)]
        pixel = [pixel[c] + offset * color[c] for c in range(3)]
        start = start + depth
    first = owner[0] * (OWNED * LANES)
    error = []
    for c in range(3):
        rows = [
            target[c : c + 1, pl.ds(pl.multiple_of(first + k * LANES, LANES), LANES)]
            for k in range(OWNED)
        ]
        error.append(pixel[c] - jnp.concatenate(rows, axis=0))
    residual = [2.0 * e for e in error]
    loss = error[0] * error[0] + error[1] * error[1] + error[2] * error[2]
    loss = jnp.sum(loss, axis=0, keepdims=True)
    previous = zero
    for s in range(SLABS):
        left = [residual[c] * (pixel[c] - befores[s][c]) for c in range(3)]
        left = left[0] + left[1] + left[2]
        answer = [offsets[s] * residual[c] for c in range(3)] + [left]
        if s % 2 == 0:
            answer += [0.5 * (left - previous)]
        else:
            last = [residual[c] * ends[s][c] for c in range(3)]
            previous = last[0] + last[1] + last[2] - left
            answer += [0.5 * (left - previous)]
        top = s * ANSWER
        for q, part in enumerate(answer):
            out[top + q * OWNED : top + (q + 1) * OWNED, :] = part
        out[top + LOSS : top + ANSWER, :] = loss


def scan_slabs(owner, slabs, target):
    return call(
        scan_kernel,
        "scan_slabs",
        [pl.BlockSpec(memory_space=pltpu.SMEM), WHOLE, WHOLE],
        WHOLE,
        jax.ShapeDtypeStruct((SLABS * ANSWER, LANES), F32),
        [],
        6,
    )(owner, slabs, target)


def halves_kernel(slab, density_in, radiance_in, rim, near, far, density, radiance, held, sems, out_sems):
    even = slab[0] % 2 == 0
    odd_share = jnp.where(even, 0.0, 0.25)

    def one_group(out, first, group, carry):
        base = pl.multiple_of(group * GROUP, GROUP)
        here = sample_row(density, 0, 0, base)
        rows = pl.ds(base, GROUP)
        color = [sample_row(radiance, c, 0, base) for c in range(3)]
        beside = [rim[1 + c, rows, :] for c in range(3)]
        before = color
        doubled = jnp.zeros((GROUP, LANES), F32)
        half = None
        for i in range(SAMPLES):
            last = i == SAMPLES - 1
            after = beside if last else [sample_row(radiance, c, i + 1, base) for c in range(3)]
            if i == 0:
                new = [0.25 * (color[c] + after[c]) for c in range(3)]
                store = [new[c] + odd_share * (beside[c] + color[c]) for c in range(3)]
            else:
                transmit = 0.25 * jnp.exp(-0.5 * doubled)
                new = [half[c] + transmit * (after[c] - before[c]) for c in range(3)]
                if last:
                    new = [jnp.where(even, new[c], 0.0) for c in range(3)]
                store = [half[c] + new[c] for c in range(3)]
            for c in range(3):
                out[c * EIGHTS + i // 8, sample_place(i, base - first), :] = store[c]
            if not last:
                nxt = sample_row(density, 0, i + 1, base)
                doubled = doubled + (here + nxt)
                here = nxt
            before, color, half = color, after, new
        return carry

    arrivals = fetches([(density_in, density), (radiance_in, radiance)], sems)
    departures = fetches([(held, far)], out_sems)
    start_all(arrivals)
    each = TILES // GROUP // len(arrivals)
    kept = NEAR // GROUP // each
    for k, some in enumerate(arrivals):
        wait_all([some])
        out, first = (near, 0) if k < kept else (held, NEAR)
        lax.fori_loop(k * each, (k + 1) * each, functools.partial(one_group, out, first), 0)
        if k >= kept:
            start_all([departures[k - kept]])
    wait_all(departures)


def halves_of(slab, density, radiance, rim, chunks=8):
    far = (3 * EIGHTS, (TILES - NEAR) * 8, LANES)
    return call(
        halves_kernel,
        "slab_halves",
        [pl.BlockSpec(memory_space=pltpu.SMEM), FAR, FAR, WHOLE],
        [WHOLE, FAR],
        [
            jax.ShapeDtypeStruct((3 * EIGHTS, NEAR * 8, LANES), F32),
            jax.ShapeDtypeStruct(far, F32),
        ],
        [
            pltpu.VMEM((EIGHTS, TILES * 8, LANES), F32),
            pltpu.VMEM((3 * EIGHTS, TILES * 8, LANES), F32),
            pltpu.VMEM(far, F32),
            pltpu.SemaphoreType.DMA((chunks, 2)),
            pltpu.SemaphoreType.DMA((chunks * (TILES - NEAR) // TILES, 1)),
        ],
        HALVES_MIB,
        1_000_000_000,
    )(slab, density, radiance, rim)


def loss_kernel(back, near, out, near_out):
    total = jnp.sum(back[pl.ds(LOSS, SLABS, stride=ANSWER), :], axis=0, keepdims=True)
    for z in range(out.shape[0]):
        out[z] = total


def tile_loss(back, near, count):
    return pl.pallas_call(
        loss_kernel,
        in_specs=[WHOLE, WHOLE],
        out_specs=[WHOLE, WHOLE],
        out_shape=[
            jax.ShapeDtypeStruct((count, 1, LANES), F32),
            jax.ShapeDtypeStruct(near.shape, F32),
        ],
        input_output_aliases={1: 1},
        compiler_params=pltpu.CompilerParams(vmem_limit_bytes=8 * MIB),
        cost_estimate=pl.CostEstimate(flops=0, bytes_accessed=1024, transcendentals=0),
        name="tile_loss",
    )(back, near)


def gradient_kernel(slab, near, far_in, back, out, far, held, sems, out_sems):
    sample = lax.broadcasted_iota(jnp.int32, (8, LANES), 0)
    even = slab[0] % 2 == 0
    top = sample == jnp.where(even, 0, 8)
    bottom = sample == jnp.where(even, 8, 7)

    def one_owner(halves, first, owner, carry):
        for k in range(OWNED):
            tile = owner * OWNED + k
            rows = pl.ds(pl.multiple_of(tile * 8, 8), 8)
            from_rows = pl.ds(pl.multiple_of((tile - first) * 8, 8), 8)
            known = [
                jnp.broadcast_to(back[pl.ds(owner * ANSWER + q * OWNED + k, 1), :], (8, LANES))
                for q in range(5)
            ]
            for a in range(EIGHTS):
                value = known[0] * halves[a, from_rows, :]
                value += known[1] * halves[EIGHTS + a, from_rows, :]
                value += known[2] * halves[2 * EIGHTS + a, from_rows, :]
                left = known[3]
                if a == 0:
                    left = jnp.where(top, known[4], left)
                if a == EIGHTS - 1:
                    left = jnp.where(bottom, known[4], left)
                held[a, rows, :] = value - left
        return carry

    arrivals = fetches([(far_in, far)], sems)
    departures = fetches([(held, out)], out_sems)
    start_all(arrivals)
    each = SLABS // len(departures)
    kept = len(departures) - len(arrivals)
    for k, some in enumerate(departures):
        if k >= kept:
            wait_all([arrivals[k - kept]])
        halves, first = (near, 0) if k < kept else (far, NEAR)
        lax.fori_loop(k * each, (k + 1) * each, functools.partial(one_owner, halves, first), 0)
        start_all([some])
    wait_all(departures)


def gradient(slab, near, far, back, chunks=8):
    shape = (EIGHTS, TILES * 8, LANES)
    return call(
        gradient_kernel,
        "slab_gradient",
        [pl.BlockSpec(memory_space=pltpu.SMEM), WHOLE, FAR, WHOLE],
        FAR,
        jax.ShapeDtypeStruct(shape, F32),
        [
            pltpu.VMEM((3 * EIGHTS, (TILES - NEAR) * 8, LANES), F32),
            pltpu.VMEM(shape, F32),
            pltpu.SemaphoreType.DMA((chunks * (TILES - NEAR) // TILES, 1)),
            pltpu.SemaphoreType.DMA((chunks, 1)),
        ],
        GRADIENT_MIB,
        1_000_000_000,
    )(slab, near, far, back)


def on_device(density, radiance, target):
    density, radiance = tiled_view(density), tiled_view(radiance)
    owner = lax.axis_index("depth").astype(jnp.int32)[None]
    known, edge = inner(owner, density, radiance)
    rim = lax.ppermute(edge, "depth", [(s, s ^ 1) for s in range(SLABS)])
    slabs = lax.all_to_all(closing(owner, known, rim), "depth", 0, 0, tiled=True)
    answers = scan_slabs(owner, slabs, target)
    answers = answers.reshape(SLABS, ANSWER, 1, LANES)
    back = lax.all_to_all(answers, "depth", 0, 0, tiled=True).reshape(SLABS * ANSWER, LANES)
    near, far = halves_of(owner, density, radiance, rim)
    zs = lax.axis_size("rays")
    tile, near = tile_loss(back, near, zs)
    losses = lax.all_to_all(tile, "rays", 0, 0, tiled=True)
    grad = gradient(owner, near, far, back)
    loss_mean = jnp.sum(losses) / (3.0 * zs * TILES * LANES)
    return untiled_view(grad), loss_mean


def solution(mesh):
    in_specs = (P("depth", "rays"), P(None, "depth", "rays"), P(None, "rays"))
    out_specs = (P("depth", "rays"), P())
    return jax.shard_map(
        on_device, mesh=mesh, in_specs=in_specs, out_specs=out_specs, check_vma=False
    )
```

```python
import jax
import jax.numpy as jnp
from jax import lax
from jax.experimental import pallas as pl
from jax.experimental.pallas import tpu as pltpu
from jax.sharding import PartitionSpec as P

SLABS = 32
SAMPLES = 32
EIGHTS = SAMPLES // 8
TILES = 128
LANES = 128
OWNED = TILES // SLABS
GROUP = 8
KNOWN = 12
SENT = 8
LOSS = 5 * OWNED
ANSWER = LOSS + 1
F32 = jnp.float32
MIB = 1 << 20
INNER_MIB, GRADIENT_MIB = 52, 52
WHOLE = pl.BlockSpec(memory_space=pltpu.VMEM)
FAR = pl.BlockSpec(memory_space=pltpu.HBM)


def call(kernel, name, in_specs, out_specs, out_shape, scratch, mib, flops=0):
    return pl.pallas_call(
        kernel,
        in_specs=in_specs,
        out_specs=out_specs,
        out_shape=out_shape,
        scratch_shapes=scratch,
        compiler_params=pltpu.CompilerParams(vmem_limit_bytes=int(mib * MIB)),
        cost_estimate=pl.CostEstimate(flops=flops, bytes_accessed=1024, transcendentals=0),
        name=name,
    )


def tiled_view(block):
    lead = block.shape[:-2]
    cut = block.reshape(*lead, EIGHTS, 8, TILES, LANES)
    return jnp.swapaxes(cut, -3, -2).reshape(-1, TILES * 8, LANES)


def untiled_view(block):
    cut = block.reshape(EIGHTS, TILES, 8, LANES)
    return jnp.swapaxes(cut, 1, 2).reshape(SAMPLES, TILES * LANES)


def sample_place(sample, base):
    return pl.ds(pl.multiple_of(base * 8, 64) + sample % 8, GROUP, stride=8)


def sample_row(ref, channel, sample, base):
    return ref[channel * EIGHTS + sample // 8, sample_place(sample, base), :]


def fetches(pairs, sems):
    chunks = sems.shape[0]
    size = pairs[0][0].shape[1] // chunks
    return [
        [
            pltpu.make_async_copy(a.at[:, pl.ds(k * size, size)], b.at[:, pl.ds(k * size, size)], sems.at[k, n])
            for n, (a, b) in enumerate(pairs)
        ]
        for k in range(chunks)
    ]


def start_all(copies):
    for some in copies:
        for copy in some:
            copy.start()


def wait_all(copies):
    for some in copies:
        for copy in some:
            copy.wait()


def in_chunks(arrivals, departures, count, one):
    start_all(arrivals)
    each = count // len(arrivals)
    for k, some in enumerate(arrivals):
        wait_all([some])
        lax.fori_loop(k * each, (k + 1) * each, one, 0)
        if departures:
            start_all([departures[k]])
    if departures:
        wait_all(departures)


def inner_kernel(slab, density_in, radiance_in, out, edge, density, radiance, sems):
    odd = slab[0] % 2 == 1
    def one_group(group, carry):
        base = pl.multiple_of(group * GROUP, GROUP)
        first = here = sample_row(density, 0, 0, base)
        color = [sample_row(radiance, c, 0, base) for c in range(3)]
        before = first_color = color
        doubled = jnp.zeros((GROUP, LANES), F32)
        total = None
        half = None
        for i in range(SAMPLES - 1):
            nxt = sample_row(density, 0, i + 1, base)
            after = [sample_row(radiance, c, i + 1, base) for c in range(3)]
            if i == 0:
                total = [0.5 * (color[c] + after[c]) for c in range(3)]
            else:
                total = [total[c] + half * (after[c] - before[c]) for c in range(3)]
            doubled = doubled + (here + nxt)
            half = 0.5 * jnp.exp(-0.5 * doubled)
            before, color, here = color, after, nxt
        known = [total[c] - half * before[c] for c in range(3)]
        rows = pl.ds(base, GROUP)
        for q, part in enumerate([doubled, here, first] + known + color + first_color):
            out[q, rows, :] = part
        edge[0, rows, :] = first
        for c in range(3):
            edge[1 + c, rows, :] = jnp.where(odd, first_color[c], color[c])
        return carry

    arrivals = fetches([(density_in, density), (radiance_in, radiance)], sems)
    in_chunks(arrivals, None, TILES // GROUP, one_group)


def inner(slab, density, radiance, chunks=8):
    return call(
        inner_kernel,
        "slab_inner",
        [pl.BlockSpec(memory_space=pltpu.SMEM), FAR, FAR],
        [WHOLE, WHOLE],
        [
            jax.ShapeDtypeStruct((KNOWN, TILES, LANES), F32),
            jax.ShapeDtypeStruct((4, TILES, LANES), F32),
        ],
        [
            pltpu.VMEM((EIGHTS, TILES * 8, LANES), F32),
            pltpu.VMEM((3 * EIGHTS, TILES * 8, LANES), F32),
            pltpu.SemaphoreType.DMA((chunks, 2)),
        ],
        INNER_MIB,
    )(slab, density, radiance)


def closing_kernel(slab, known, rim, out):
    def send(parity, parts_of):
        @pl.when(slab[0] % 2 == parity)
        def _():
            for group in range(TILES // GROUP):
                rows = pl.ds(group * GROUP, GROUP)
                for q, part in enumerate(parts_of(rows)):
                    for k in range(GROUP // OWNED):
                        owner = group * (GROUP // OWNED) + k
                        out[owner, q * OWNED : (q + 1) * OWNED, :] = part[k * OWNED : (k + 1) * OWNED, :]

    def even(rows):
        part = [known[q, rows, :] for q in range(KNOWN)]
        after = [rim[1 + c, rows, :] for c in range(3)]
        depth = 0.5 * (part[0] + part[1] + rim[0, rows, :])
        half = 0.5 * jnp.exp(-0.5 * part[0])
        behind = 0.5 * jnp.exp(-depth)
        color = [part[3 + c] + half * after[c] - behind * (part[6 + c] + after[c]) for c in range(3)]
        return [depth] + color + [part[2]] + part[9:]

    def odd(rows):
        return [known[q, rows, :] for q in (0, 3, 4, 5, 1, 6, 7, 8)]

    send(0, even)
    send(1, odd)


def closing(slab, known, rim):
    return call(
        closing_kernel,
        "slab_closing",
        [pl.BlockSpec(memory_space=pltpu.SMEM), WHOLE, WHOLE],
        WHOLE,
        jax.ShapeDtypeStruct((SLABS, SENT * OWNED, LANES), F32),
        [],
        6,
    )(slab, known, rim)


def scan_kernel(owner, slabs, target, out):
    def value(s, q):
        return slabs[s, q * OWNED : (q + 1) * OWNED, :]

    zero = jnp.zeros((OWNED, LANES), F32)
    start = zero
    pixel = [zero] * 3
    offsets, befores, ends = [], [], []
    for s in range(SLABS):
        offset = jnp.exp(-start)
        offsets.append(offset)
        befores.append(pixel)
        color = [value(s, 1 + c) for c in range(3)]
        if s % 2 == 0:
            depth = value(s, 0)
            ends.append(None)
        else:
            more = s < SLABS - 1
            depth = 0.5 * (value(s, 0) + value(s, 4) + (value(s + 1, 4) if more else zero))
            half = 0.5 * jnp.exp(-0.5 * value(s, 0))
            behind = 0.5 * jnp.exp(-depth)
            after = [value(s + 1, 5 + c) if more else zero for c in range(3)]
            color = [color[c] + half * after[c] for c in range(3)]
            ends.append([offset * color[c] for c in range(3)])
            color = [color[c] - behind * (value(s, 5 + c) + after[c]) for c in range(3)]
        pixel = [pixel[c] + offset * color[c] for c in range(3)]
        start = start + depth
    first = owner[0] * (OWNED * LANES)
    error = []
    for c in range(3):
        rows = [
            target[c : c + 1, pl.ds(pl.multiple_of(first + k * LANES, LANES), LANES)]
            for k in range(OWNED)
        ]
        error.append(pixel[c] - jnp.concatenate(rows, axis=0))
    residual = [2.0 * e for e in error]
    loss = error[0] * error[0] + error[1] * error[1] + error[2] * error[2]
    loss = jnp.sum(loss, axis=0, keepdims=True)
    previous = zero
    for s in range(SLABS):
        left = [residual[c] * (pixel[c] - befores[s][c]) for c in range(3)]
        left = left[0] + left[1] + left[2]
        answer = [offsets[s] * residual[c] for c in range(3)] + [left]
        if s % 2 == 0:
            answer += [0.5 * (left - previous)]
        else:
            last = [residual[c] * ends[s][c] for c in range(3)]
            previous = last[0] + last[1] + last[2] - left
            answer += [0.5 * (left - previous)]
        top = s * ANSWER
        for q, part in enumerate(answer):
            out[top + q * OWNED : top + (q + 1) * OWNED, :] = part
        out[top + LOSS : top + ANSWER, :] = loss


def scan_slabs(owner, slabs, target):
    return call(
        scan_kernel,
        "scan_slabs",
        [pl.BlockSpec(memory_space=pltpu.SMEM), WHOLE, WHOLE],
        WHOLE,
        jax.ShapeDtypeStruct((SLABS * ANSWER, LANES), F32),
        [],
        6,
    )(owner, slabs, target)


def loss_kernel(back, out):
    total = jnp.sum(back[pl.ds(LOSS, SLABS, stride=ANSWER), :], axis=0, keepdims=True)
    for z in range(out.shape[0]):
        out[z] = total


def tile_loss(back, count):
    return call(
        loss_kernel,
        "tile_loss",
        [WHOLE],
        WHOLE,
        jax.ShapeDtypeStruct((count, 1, LANES), F32),
        [],
        4,
    )(back)


def gradient_kernel(
    slab, density_in, radiance_in, rim, back, out, density, radiance, held, sems, out_sems
):
    even = slab[0] % 2 == 0

    def one_group(group, carry):
        base = pl.multiple_of(group * GROUP, GROUP)
        rows = pl.ds(base, GROUP)

        def answer(q):
            pair = [
                back[pl.ds((group * (GROUP // OWNED) + k) * ANSWER + q * OWNED, OWNED), :]
                for k in range(GROUP // OWNED)
            ]
            return jnp.concatenate(pair, axis=0)

        scale = [answer(c) for c in range(3)]
        left, edge = answer(3), answer(4)

        def seen(colors):
            return scale[0] * colors[0] + scale[1] * colors[1] + scale[2] * colors[2]

        beside = seen([rim[1 + c, rows, :] for c in range(3)])
        color = seen([sample_row(radiance, c, 0, base) for c in range(3)])
        here = sample_row(density, 0, 0, base)
        before = color
        doubled = jnp.zeros((GROUP, LANES), F32)
        half = None
        for i in range(SAMPLES):
            last = i == SAMPLES - 1
            after = beside if last else seen([sample_row(radiance, c, i + 1, base) for c in range(3)])
            if i == 0:
                new = 0.25 * (color + after)
                store = new + jnp.where(even, -edge, 0.25 * (beside + color) - left)
            else:
                new = half + 0.25 * jnp.exp(-0.5 * doubled) * (after - before)
                store = half + (jnp.where(even, new - left, -edge) if last else new - left)
            held[i // 8, sample_place(i, base), :] = store
            if not last:
                nxt = sample_row(density, 0, i + 1, base)
                doubled = doubled + (here + nxt)
                here = nxt
            before, color, half = color, after, new
        return carry

    arrivals = fetches([(density_in, density), (radiance_in, radiance)], sems)
    in_chunks(arrivals, fetches([(held, out)], out_sems), TILES // GROUP, one_group)


def gradient(slab, density, radiance, rim, back, chunks=8):
    shape = (EIGHTS, TILES * 8, LANES)
    return call(
        gradient_kernel,
        "slab_gradient",
        [pl.BlockSpec(memory_space=pltpu.SMEM), FAR, FAR, WHOLE, WHOLE],
        FAR,
        jax.ShapeDtypeStruct(shape, F32),
        [
            pltpu.VMEM(shape, F32),
            pltpu.VMEM((3 * EIGHTS, TILES * 8, LANES), F32),
            pltpu.VMEM(shape, F32),
            pltpu.SemaphoreType.DMA((chunks, 2)),
            pltpu.SemaphoreType.DMA((chunks, 1)),
        ],
        GRADIENT_MIB,
        1_000_000_000,
    )(slab, density, radiance, rim, back)


def on_device(density, radiance, target):
    density, radiance = tiled_view(density), tiled_view(radiance)
    owner = lax.axis_index("depth").astype(jnp.int32)[None]
    known, edge = inner(owner, density, radiance)
    rim = lax.ppermute(edge, "depth", [(s, s ^ 1) for s in range(SLABS)])
    slabs = lax.all_to_all(closing(owner, known, rim), "depth", 0, 0, tiled=True)
    answers = scan_slabs(owner, slabs, target)
    answers = answers.reshape(SLABS, ANSWER, 1, LANES)
    back = lax.all_to_all(answers, "depth", 0, 0, tiled=True).reshape(SLABS * ANSWER, LANES)
    zs = lax.axis_size("rays")
    tile = tile_loss(back, zs)
    losses = lax.all_to_all(tile, "rays", 0, 0, tiled=True)
    grad = gradient(owner, density, radiance, rim, back)
    loss_mean = jnp.sum(losses) / (3.0 * zs * TILES * LANES)
    return untiled_view(grad), loss_mean


def solution(mesh):
    in_specs = (P("depth", "rays"), P(None, "depth", "rays"), P(None, "rays"))
    out_specs = (P("depth", "rays"), P())
    return jax.shard_map(
        on_device, mesh=mesh, in_specs=in_specs, out_specs=out_specs, check_vma=False
    )
```

```python
import jax
import jax.numpy as jnp
from jax import lax
from jax.experimental import pallas as pl
from jax.experimental.pallas import tpu as pltpu
from jax.sharding import PartitionSpec as P


SLABS = 32
SAMPLES = 32
EIGHTS = SAMPLES // 8
TILES = 128
LANES = 128
OWNED = TILES // SLABS
GROUP = 8
KNOWN = 12
SENT = 6
LOSS = 3 * OWNED
ANSWER = LOSS + 1
F32 = jnp.float32
MIB = 1 << 20
INNER_MIB, GRADIENT_MIB = 52, 52
WHOLE = pl.BlockSpec(memory_space=pltpu.VMEM)
FAR = pl.BlockSpec(memory_space=pltpu.HBM)


def call(kernel, in_specs, out_specs, out_shape, scratch, mib, flops=0):
    return pl.pallas_call(
        kernel,
        in_specs=in_specs,
        out_specs=out_specs,
        out_shape=out_shape,
        scratch_shapes=scratch,
        compiler_params=pltpu.CompilerParams(vmem_limit_bytes=int(mib * MIB)),
        cost_estimate=pl.CostEstimate(flops=flops, bytes_accessed=1024, transcendentals=0),
    )


def tiled_view(block):
    lead = block.shape[:-2]
    cut = block.reshape(*lead, EIGHTS, 8, TILES, LANES)
    return jnp.swapaxes(cut, -3, -2).reshape(-1, TILES * 8, LANES)


def untiled_view(block):
    cut = block.reshape(EIGHTS, TILES, 8, LANES)
    return jnp.swapaxes(cut, 1, 2).reshape(SAMPLES, TILES * LANES)


def sample_place(sample, base):
    return pl.ds(pl.multiple_of(base * 8, 64) + sample % 8, GROUP, stride=8)


def sample_row(ref, channel, sample, base):
    return ref[channel * EIGHTS + sample // 8, sample_place(sample, base), :]


def fetches(pairs, sems):
    chunks = sems.shape[0]
    size = pairs[0][0].shape[1] // chunks
    return [
        [
            pltpu.make_async_copy(a.at[:, pl.ds(k * size, size)], b.at[:, pl.ds(k * size, size)], sems.at[k, n])
            for n, (a, b) in enumerate(pairs)
        ]
        for k in range(chunks)
    ]


def start_all(copies):
    for some in copies:
        for copy in some:
            copy.start()


def wait_all(copies):
    for some in copies:
        for copy in some:
            copy.wait()


def in_chunks(arrivals, departures, count, one):
    start_all(arrivals)
    each = count // len(arrivals)
    for k, some in enumerate(arrivals):
        wait_all([some])
        lax.fori_loop(k * each, (k + 1) * each, one, 0, unroll=True)
        if departures:
            start_all([departures[k]])
    if departures:
        wait_all(departures)


def inner_kernel(slab, density_in, radiance_in, out, edge, density, radiance, sems):
    odd = slab[0] % 2 == 1

    def one_group(group, carry):
        base = pl.multiple_of(group * GROUP, GROUP)
        first = here = sample_row(density, 0, 0, base)
        color = [sample_row(radiance, c, 0, base) for c in range(3)]
        before = first_color = color
        doubled = jnp.zeros((GROUP, LANES), F32)
        total = None
        half = None
        for i in range(SAMPLES - 1):
            nxt = sample_row(density, 0, i + 1, base)
            after = [sample_row(radiance, c, i + 1, base) for c in range(3)]
            if i == 0:
                total = [0.5 * (color[c] + after[c]) for c in range(3)]
            else:
                total = [total[c] + half * (after[c] - before[c]) for c in range(3)]
            doubled = doubled + (here + nxt)
            half = 0.5 * jnp.exp(-0.5 * doubled)
            before, color, here = color, after, nxt
        known = [total[c] - half * before[c] for c in range(3)]
        rows = pl.ds(base, GROUP)
        for q, part in enumerate([doubled, here, first] + known + color + first_color):
            out[q, rows, :] = part
        edge[0, rows, :] = first
        for c in range(3):
            edge[1 + c, rows, :] = jnp.where(odd, first_color[c], color[c])
        edge[4, rows, :] = jnp.where(odd, doubled, first_color[0])
        edge[5, rows, :] = jnp.where(odd, known[0], first_color[1])
        edge[6, rows, :] = known[1]
        edge[7, rows, :] = known[2]
        return carry

    arrivals = fetches([(density_in, density), (radiance_in, radiance)], sems)
    in_chunks(arrivals, None, TILES // GROUP, one_group)


def inner(slab, density, radiance, chunks=8):
    return call(
        inner_kernel,
        [pl.BlockSpec(memory_space=pltpu.SMEM), FAR, FAR],
        [WHOLE, WHOLE],
        [
            jax.ShapeDtypeStruct((KNOWN, TILES, LANES), F32),
            jax.ShapeDtypeStruct((8, TILES, LANES), F32),
        ],
        [
            pltpu.VMEM((EIGHTS, TILES * 8, LANES), F32),
            pltpu.VMEM((3 * EIGHTS, TILES * 8, LANES), F32),
            pltpu.SemaphoreType.DMA((chunks, 2)),
        ],
        INNER_MIB,
    )(slab, density, radiance)


def closing_kernel(slab, known, rim, out, own):
    def send(parity, parts_of):
        @pl.when(slab[0] % 2 == parity)
        def _():
            for group in range(TILES // GROUP):
                rows = pl.ds(group * GROUP, GROUP)
                for q, part in enumerate(parts_of(rows)):
                    for k in range(GROUP // OWNED):
                        owner = group * (GROUP // OWNED) + k
                        out[owner, q * OWNED : (q + 1) * OWNED, :] = part[k * OWNED : (k + 1) * OWNED, :]

    def even(rows):
        part = [known[q, rows, :] for q in range(KNOWN)]
        after = [rim[1 + c, rows, :] for c in range(3)]
        doubled = part[0] + part[1] + rim[0, rows, :]
        half = 0.5 * jnp.exp(-0.5 * part[0])
        through = jnp.exp(-0.5 * doubled)
        own[0, rows, :] = through
        both = []
        for c in range(3):
            color = part[3 + c] + half * after[c] - 0.5 * through * (part[6 + c] + after[c])
            own[1 + c, rows, :] = color
            both.append(color + through * rim[5 + c, rows, :])
        return [doubled + rim[4, rows, :]] + both + [part[2], part[11]]

    def odd(rows):
        return [known[q, rows, :] for q in (1, 6, 7, 8)] + [rim[q, rows, :] for q in (4, 5)]

    send(0, even)
    send(1, odd)


def closing(slab, known, rim):
    return call(
        closing_kernel,
        [pl.BlockSpec(memory_space=pltpu.SMEM), WHOLE, WHOLE],
        [WHOLE, WHOLE],
        [
            jax.ShapeDtypeStruct((SLABS, SENT * OWNED, LANES), F32),
            jax.ShapeDtypeStruct((4, TILES, LANES), F32),
        ],
        [],
        6,
    )(slab, known, rim)


def scan_kernel(owner, slabs, target, out):
    def value(s, q):
        return slabs[s, q * OWNED : (q + 1) * OWNED, :]

    zero = jnp.zeros((OWNED, LANES), F32)
    start = zero
    pixel = [zero] * 3
    offsets, befores, ends = [], [], []
    for even in range(0, SLABS, 2):
        odd, following = even + 1, even + 2
        more = following < SLABS
        doubled = value(even, 0)
        depth = 0.5 * (doubled + value(odd, 0) + (value(following, 4) if more else zero))
        places = ((following + 1, 4), (following + 1, 5), (following, 5))
        after = [value(*place) if more else zero for place in places]
        half = 0.5 * jnp.exp(-0.5 * doubled)
        behind = 0.5 * jnp.exp(-depth)
        offset = jnp.exp(-start)
        offsets.append(offset)
        befores.append(pixel)
        last = [value(even, 1 + c) + half * after[c] for c in range(3)]
        ends.append([offset * last[c] for c in range(3)])
        pixel = [
            pixel[c] + offset * (last[c] - behind * (value(odd, 1 + c) + after[c])) for c in range(3)
        ]
        start = start + depth
    first = owner[0] * (OWNED * LANES)
    error = []
    for c in range(3):
        rows = [
            target[c : c + 1, pl.ds(pl.multiple_of(first + k * LANES, LANES), LANES)]
            for k in range(OWNED)
        ]
        error.append(pixel[c] - jnp.concatenate(rows, axis=0))
    residual = [2.0 * e for e in error]
    loss = error[0] * error[0] + error[1] * error[1] + error[2] * error[2]
    loss = jnp.sum(loss, axis=0, keepdims=True)
    previous = zero
    for chip in range(SLABS // 2):
        left = [residual[c] * (pixel[c] - befores[chip][c]) for c in range(3)]
        left = left[0] + left[1] + left[2]
        last = [residual[c] * ends[chip][c] for c in range(3)]
        last = last[0] + last[1] + last[2] - left
        answers = [offsets[chip] * residual[c] for c in range(3)]
        answers = [answers, [left, 0.5 * (left - previous), last]]
        previous = last
        for parity, answer in enumerate(answers):
            top = (2 * chip + parity) * ANSWER
            for q, part in enumerate(answer):
                out[top + q * OWNED : top + (q + 1) * OWNED, :] = part
            out[top + LOSS : top + ANSWER, :] = loss


def scan_slabs(owner, slabs, target):
    return call(
        scan_kernel,
        [pl.BlockSpec(memory_space=pltpu.SMEM), WHOLE, WHOLE],
        WHOLE,
        jax.ShapeDtypeStruct((SLABS * ANSWER, LANES), F32),
        [],
        6,
    )(owner, slabs, target)


def loss_kernel(back, out):
    total = jnp.sum(back[pl.ds(LOSS, SLABS, stride=ANSWER), :], axis=0, keepdims=True)
    for z in range(out.shape[0]):
        out[z] = total


def tile_loss(back, count):
    return call(loss_kernel, [WHOLE], WHOLE, jax.ShapeDtypeStruct((count, 1, LANES), F32), [], 4)(back)


def answer_rows(back, group, q):
    each = GROUP // OWNED
    pair = [back[pl.ds((group * each + k) * ANSWER + q * OWNED, OWNED), :] for k in range(each)]
    return jnp.concatenate(pair, axis=0)


def share_kernel(slab, back, own, out):
    def give(parity, parts_of):
        @pl.when(slab[0] % 2 == parity)
        def _():
            for group in range(TILES // GROUP):
                rows = pl.ds(group * GROUP, GROUP)
                for q, part in enumerate(parts_of(group, rows)):
                    out[q, rows, :] = part

    def even(group, rows):
        scale = [answer_rows(back, group, c) for c in range(3)]
        seen = [scale[c] * own[1 + c, rows, :] for c in range(3)]
        return [own[0, rows, :] * scale[c] for c in range(3)] + [seen[0] + seen[1] + seen[2]]

    def odd(group, rows):
        return [answer_rows(back, group, q) for q in (0, 1, 0, 1)]

    give(0, even)
    give(1, odd)


def share(slab, back, own):
    return call(
        share_kernel,
        [pl.BlockSpec(memory_space=pltpu.SMEM), WHOLE, WHOLE],
        WHOLE,
        jax.ShapeDtypeStruct((4, TILES, LANES), F32),
        [],
        6,
    )(slab, back, own)


def gradient_kernel(
    slab, density_in, radiance_in, rim, back, shared, out, density, radiance, held, sems, out_sems
):
    even = slab[0] % 2 == 0

    def one_group(group, carry):
        base = pl.multiple_of(group * GROUP, GROUP)
        rows = pl.ds(base, GROUP)

        given = [shared[q, rows, :] for q in range(4)]
        answer = [answer_rows(back, group, q) for q in range(3)]
        scale = [jnp.where(even, answer[c], given[c]) for c in range(3)]
        left = jnp.where(even, given[0], answer[0] - given[3])
        edge = jnp.where(even, given[1], 0.5 * (left - answer[2]))

        def seen(colors):
            return scale[0] * colors[0] + scale[1] * colors[1] + scale[2] * colors[2]

        beside = seen([rim[1 + c, rows, :] for c in range(3)])
        color = seen([sample_row(radiance, c, 0, base) for c in range(3)])
        here = sample_row(density, 0, 0, base)
        before = color
        doubled = jnp.zeros((GROUP, LANES), F32)
        half = None
        for i in range(SAMPLES):
            last = i == SAMPLES - 1
            after = beside if last else seen([sample_row(radiance, c, i + 1, base) for c in range(3)])
            if i == 0:
                new = 0.25 * (color + after)
                store = new + jnp.where(even, -edge, 0.25 * (beside + color) - left)
            else:
                new = half + 0.25 * jnp.exp(-0.5 * doubled) * (after - before)
                store = half + (jnp.where(even, new - left, -edge) if last else new - left)
            held[i // 8, sample_place(i, base), :] = store
            if not last:
                nxt = sample_row(density, 0, i + 1, base)
                doubled = doubled + (here + nxt)
                here = nxt
            before, color, half = color, after, new
        return carry

    arrivals = fetches([(density_in, density), (radiance_in, radiance)], sems)
    in_chunks(arrivals, fetches([(held, out)], out_sems), TILES // GROUP, one_group)


def gradient(slab, density, radiance, rim, back, shared, chunks=8):
    shape = (EIGHTS, TILES * 8, LANES)
    return call(
        gradient_kernel,
        [pl.BlockSpec(memory_space=pltpu.SMEM), FAR, FAR, WHOLE, WHOLE, WHOLE],
        FAR,
        jax.ShapeDtypeStruct(shape, F32),
        [
            pltpu.VMEM(shape, F32),
            pltpu.VMEM((3 * EIGHTS, TILES * 8, LANES), F32),
            pltpu.VMEM(shape, F32),
            pltpu.SemaphoreType.DMA((chunks, 2)),
            pltpu.SemaphoreType.DMA((chunks, 1)),
        ],
        GRADIENT_MIB,
        1_000_000_000,
    )(slab, density, radiance, rim, back, shared)


def one_slab(density, radiance, target):
    density, radiance = tiled_view(density), tiled_view(radiance)
    owner = lax.axis_index("depth").astype(jnp.int32)[None]
    known, edge = inner(owner, density, radiance)
    swap = [(s, s ^ 1) for s in range(SLABS)]
    rim = lax.ppermute(edge, "depth", swap)
    sent, own = closing(owner, known, rim)
    slabs = lax.all_to_all(sent, "depth", 0, 0, tiled=True)
    answers = scan_slabs(owner, slabs, target)
    answers = answers.reshape(SLABS, ANSWER, 1, LANES)
    back = lax.all_to_all(answers, "depth", 0, 0, tiled=True).reshape(SLABS * ANSWER, LANES)
    zs = lax.axis_size("rays")
    tile = tile_loss(back, zs)
    losses = lax.all_to_all(tile, "rays", 0, 0, tiled=True)
    given = share(owner, back, own)
    shared = lax.ppermute(given, "depth", swap)
    grad = gradient(owner, density, radiance, rim, back, shared)
    loss_mean = jnp.sum(losses) / (3.0 * zs * TILES * LANES)
    return untiled_view(grad), loss_mean


def solution(mesh):
    in_specs = (P("depth", "rays"), P(None, "depth", "rays"), P(None, "rays"))
    out_specs = (P("depth", "rays"), P())
    return jax.shard_map(one_slab, mesh=mesh, in_specs=in_specs, out_specs=out_specs, check_vma=False)
```
